64 devices in a mesh: batch: 4 (over x, y), dap: 16 (over z, core).
Axes of the slice: x: 2, y: 2, z: 8, core: 2. Of those that a mesh axis runs over, the one named last changes fastest.
The devices are a block of a 4x4x8 slice.
Arguments:
- z_pair: bfloat16 [1536, 384, 128], P(('batch', 'dap')), parts along dimension 0
- pair_mask: int32 [1536, 384], P(('batch', 'dap')), parts along dimension 0
- dz_out: bfloat16 [1536, 384, 128], P(('batch', 'dap')), parts along dimension 0
- ln_in_scale: bfloat16 [128], replicated
- ln_in_offset: bfloat16 [128], replicated
- w_in: bfloat16 [128, 512], replicated
- b_in: bfloat16 [512], replicated
- ln_out_scale: bfloat16 [128], replicated
- ln_out_offset: bfloat16 [128], replicated
- w_out: bfloat16 [128, 128], replicated
- b_out: bfloat16 [128], replicated
- w_gate: bfloat16 [128, 128], replicated
- b_gate: bfloat16 [128], replicated
Outputs:
- output 1: bfloat16 [1536, 384, 128], P(('batch', 'dap')), parts along dimension 0
- output 2: bfloat16 [512], P('batch'), parts along dimension 0
- output 3: bfloat16 [512], P('batch'), parts along dimension 0
- output 4: bfloat16 [512, 512], P('batch'), parts along dimension 0
- output 5: bfloat16 [2048], P('batch'), parts along dimension 0
- output 6: bfloat16 [512], P('batch'), parts along dimension 0
- output 7: bfloat16 [512], P('batch'), parts along dimension 0
- output 8: bfloat16 [512, 128], P('batch'), parts along dimension 0
- output 9: bfloat16 [512], P('batch'), parts along dimension 0
- output 10: bfloat16 [512, 128], P('batch'), parts along dimension 0
- output 11: bfloat16 [512], P('batch'), parts along dimension 0
There are 4 independent parts. The reference program is written for one: setup_inputs(seed, part) draws one part's arguments, and reference() takes and returns one part's arrays. A program takes and returns all parts, laid end to end along the dimension named above; an argument that names none is the same for every part.
All inputs are finite; a program needn't handle non-finite values.
Results may differ from the reference program's by a relative error of at most 0.0194336.
Values are sent between devices in bfloat16 or wider.
A program may use at most 768 MiB of HBM per device.

```python
import functools
import jax
import jax.numpy as jnp
from jax import lax

N = 384
CZ = 128
CH = 128
LN_EPS = 1e-5


@jax.custom_vjp
def dense_map(x_act, w_mat):
    return jnp.einsum('...k,km->...m', x_act.astype(jnp.float32), w_mat.astype(jnp.float32))


def dense_fwd(x_act, w_mat):
    return dense_map(x_act, w_mat), (x_act, w_mat)


def dense_bwd(saved_res, grad_out):
    x_act, w_mat = saved_res
    grad_b16 = grad_out.astype(jnp.bfloat16).astype(jnp.float32)
    grad_x = jnp.einsum('...m,km->...k', grad_b16, w_mat.astype(jnp.float32)).astype(jnp.bfloat16)
    grad_w = jnp.einsum('...k,...m->km', x_act.astype(jnp.float32), grad_b16).astype(jnp.bfloat16)
    return grad_x, grad_w


dense_map.defvjp(dense_fwd, dense_bwd)


@jax.custom_vjp
def triangle_map(act_a, act_b):
    return jnp.einsum('ikc,jkc->ijc', act_a.astype(jnp.float32), act_b.astype(jnp.float32))


def triangle_fwd(act_a, act_b):
    return triangle_map(act_a, act_b), (act_a, act_b)


def triangle_bwd(saved_res, grad_out):
    act_a, act_b = saved_res
    grad_b16 = grad_out.astype(jnp.bfloat16).astype(jnp.float32)
    grad_a = jnp.einsum('ijc,jkc->ikc', grad_b16, act_b.astype(jnp.float32)).astype(jnp.bfloat16)
    grad_bb = jnp.einsum('ijc,ikc->jkc', grad_b16, act_a.astype(jnp.float32)).astype(jnp.bfloat16)
    return grad_a, grad_bb


triangle_map.defvjp(triangle_fwd, triangle_bwd)


def layer_norm(x_val, ln_scale, ln_offset):
    mean_val = jnp.mean(x_val, axis=-1, keepdims=True)
    centered = x_val - mean_val
    var_val = jnp.mean(centered * centered, axis=-1, keepdims=True)
    return centered * lax.rsqrt(var_val + LN_EPS) * ln_scale.astype(jnp.float32) + ln_offset.astype(jnp.float32)


def outgoing_layer(z_pair, ln_in_scale, ln_in_offset, w_in, b_in, ln_out_scale, ln_out_offset, w_out, b_out, w_gate, b_gate, pair_mask):
    z_f = z_pair.astype(jnp.float32)
    z_norm = layer_norm(z_f, ln_in_scale, ln_in_offset).astype(jnp.bfloat16)
    w_cat = jnp.concatenate([w_in, w_gate], axis=1)
    b_cat = jnp.concatenate([b_in, b_gate]).astype(jnp.float32)
    proj_all = dense_map(z_norm, w_cat) + b_cat
    mask_f = pair_mask.astype(jnp.float32)[..., None]
    proj_a = proj_all[..., :CH]
    proj_b = proj_all[..., CH:2 * CH]
    sig_a = jax.nn.sigmoid(proj_all[..., 2 * CH:3 * CH])
    sig_b = jax.nn.sigmoid(proj_all[..., 3 * CH:4 * CH])
    sig_g = jax.nn.sigmoid(proj_all[..., 4 * CH:])
    act_a = (mask_f * sig_a * proj_a).astype(jnp.bfloat16)
    act_b = (mask_f * sig_b * proj_b).astype(jnp.bfloat16)
    tri_out = triangle_map(act_a, act_b)
    o_norm = layer_norm(tri_out, ln_out_scale, ln_out_offset).astype(jnp.bfloat16)
    update = (dense_map(o_norm, w_out) + b_out.astype(jnp.float32)).astype(jnp.bfloat16)
    return (z_f + sig_g * update.astype(jnp.float32)).astype(jnp.bfloat16)


def setup_inputs(seed: int = 0, part: int = 0) -> dict:
    part_key = jax.random.fold_in(jax.random.key(seed), part)
    k_z, k_dy, k_res, k_pair = jax.random.split(part_key, 4)
    w_keys = jax.random.split(jax.random.key(seed + 1), 12)
    res_keep = (jax.random.randint(k_res, (N,), 0, 8) != 0).astype(jnp.int32)
    pair_keep = (jax.random.randint(k_pair, (N, N), 0, 16) != 0).astype(jnp.int32)
    pair_mask = res_keep[:, None] * res_keep[None, :] * pair_keep
    return {
        'z_pair': jax.random.normal(k_z, (N, N, CZ), jnp.float32).astype(jnp.bfloat16),
        'pair_mask': pair_mask,
        'dz_out': jax.random.normal(k_dy, (N, N, CZ), jnp.float32).astype(jnp.bfloat16),
        'ln_in_scale': (1.0 + 0.3 * jax.random.normal(w_keys[0], (CZ,), jnp.float32)).astype(jnp.bfloat16),
        'ln_in_offset': (0.3 * jax.random.normal(w_keys[1], (CZ,), jnp.float32)).astype(jnp.bfloat16),
        'w_in': (jax.random.normal(w_keys[2], (CZ, 4 * CH), jnp.float32) * CZ ** -0.5).astype(jnp.bfloat16),
        'b_in': (0.5 * jax.random.normal(w_keys[3], (4 * CH,), jnp.float32)).astype(jnp.bfloat16),
        'ln_out_scale': (1.0 + 0.3 * jax.random.normal(w_keys[4], (CH,), jnp.float32)).astype(jnp.bfloat16),
        'ln_out_offset': (0.3 * jax.random.normal(w_keys[5], (CH,), jnp.float32)).astype(jnp.bfloat16),
        'w_out': (jax.random.normal(w_keys[6], (CH, CZ), jnp.float32) * CH ** -0.5).astype(jnp.bfloat16),
        'b_out': (0.5 * jax.random.normal(w_keys[7], (CZ,), jnp.float32)).astype(jnp.bfloat16),
        'w_gate': (jax.random.normal(w_keys[8], (CZ, CZ), jnp.float32) * CZ ** -0.5).astype(jnp.bfloat16),
        'b_gate': (0.5 * jax.random.normal(w_keys[9], (CZ,), jnp.float32)).astype(jnp.bfloat16),
    }


def reference(z_pair, pair_mask, dz_out, ln_in_scale, ln_in_offset, w_in, b_in, ln_out_scale, ln_out_offset, w_out, b_out, w_gate, b_gate):
    layer_fn = functools.partial(outgoing_layer, pair_mask=pair_mask)
    z_next, vjp_fn = jax.vjp(layer_fn, z_pair, ln_in_scale, ln_in_offset, w_in, b_in, ln_out_scale, ln_out_offset, w_out, b_out, w_gate, b_gate)
    d_z, d_in_scale, d_in_offset, d_w_in, d_b_in, d_out_scale, d_out_offset, d_w_out, d_b_out, d_w_gate, d_b_gate = vjp_fn(dz_out)
    return (d_z, d_in_scale, d_in_offset, d_w_in, d_b_in, d_out_scale, d_out_offset, d_w_out, d_b_out, d_w_gate, d_b_gate)
```

```python
import functools
import jax
import jax.numpy as jnp
from jax import lax
from jax.experimental import pallas as pl
from jax.experimental.pallas import tpu as pltpu
from jax.sharding import PartitionSpec as P

LN_EPS = 1e-5
CHUNK = 8
F32 = jnp.float32
BF16 = jnp.bfloat16


def mm(x_val, y_val):
    return lax.dot_general(x_val, y_val, (((1,), (0,)), ((), ())), preferred_element_type=F32)


def mm_nt(x_val, y_val):
    return lax.dot_general(x_val, y_val, (((1,), (1,)), ((), ())), preferred_element_type=F32)


def mm_tn(x_val, y_val):
    return lax.dot_general(x_val, y_val, (((0,), (0,)), ((), ())), preferred_element_type=F32)


def norm_stats(x_val):
    size = x_val.shape[0]
    mean_val = jnp.sum(x_val, axis=0, keepdims=True) * (1.0 / size)
    centered = x_val - mean_val
    inv_std = lax.rsqrt(jnp.sum(centered * centered, axis=0, keepdims=True) * (1.0 / size) + LN_EPS)
    return centered * inv_std, inv_std


def norm_back(grad_hat, x_hat, inv_std):
    size = x_hat.shape[0]
    mean_grad = jnp.sum(grad_hat, axis=0, keepdims=True) * (1.0 / size)
    mean_proj = jnp.sum(grad_hat * x_hat, axis=0, keepdims=True) * (1.0 / size)
    return inv_std * (grad_hat - mean_grad - x_hat * mean_proj)


def lane_fold(x_val):
    total = x_val[:, :128]
    for tile in range(1, x_val.shape[1] // 128):
        total = total + x_val[:, tile * 128:(tile + 1) * 128]
    return total


def kernel(n_dev, z_ref, dy_ref, mask_ref, w_in_ref, w_gate_ref, w_out_ref, par_ref,
           dz_ref, gw_in_ref, gw_gate_ref, gw_out_ref, gvec_ref,
           w_in_t, w_gate_t, w_out_t, eye, cols,
           a_send, b_send, a_ch, b_ch, o_ch, o_row, do_send, do_ch, da_ch, da_row, db_ch, db_row,
           stage_a, stage_b, zn_keep, gg_keep, m_acc, v_acc, v_row, m_recv, v_recv, g_send, g_all,
           send_sem, a_sem, b_sem, o_sem, do_sem, da_sem, db_sem, m_sem, v_sem, g_sem):
    rows, num, chan = z_ref.shape
    n_chunk = rows // CHUNK
    part = chan // n_dev
    me = lax.axis_index('dap')
    shard = m_recv.shape[1]

    barrier = pltpu.get_barrier_semaphore()

    def ring_peer(step):
        half = step // 2 + 1
        offset = half + lax.rem(step, 2) * (n_dev - 2 * half)
        return lax.rem(me + offset, n_dev)

    def hello(step, carry):
        pl.semaphore_signal(barrier, inc=1, device_id={'dap': ring_peer(step)}, device_id_type=pl.DeviceIdType.MESH)
        return carry

    lax.fori_loop(0, n_dev - 1, hello, 0)

    row_id = lax.broadcasted_iota(jnp.int32, (chan, chan), 0)
    col_id = lax.broadcasted_iota(jnp.int32, (chan, chan), 1)
    eye[...] = jnp.where(row_id == col_id, 1.0, 0.0).astype(BF16)
    cols[...] = jnp.transpose(par_ref[...])
    for blk in range(4):
        w_in_t[blk * chan:(blk + 1) * chan, :] = jnp.transpose(w_in_ref[:, blk * chan:(blk + 1) * chan].astype(F32)).astype(BF16)
    w_gate_t[...] = jnp.transpose(w_gate_ref[...].astype(F32)).astype(BF16)
    w_out_t[...] = jnp.transpose(w_out_ref[...].astype(F32)).astype(BF16)
    m_acc[...] = jnp.zeros_like(m_acc)
    v_acc[...] = jnp.zeros_like(v_acc)

    def col(idx):
        return cols[:, idx:idx + 1]

    def exchange(src_of, dst_ref, send_idx, recv_sem):
        def one(step, carry):
            peer = ring_peer(step)
            pltpu.make_async_remote_copy(
                src_ref=src_of(peer), dst_ref=dst_ref, send_sem=send_sem.at[send_idx], recv_sem=recv_sem,
                device_id={'dap': peer}, device_id_type=pl.DeviceIdType.MESH).start()
            return carry
        lax.fori_loop(0, n_dev - 1, one, 0)
        pltpu.make_async_copy(src_of(me), dst_ref, recv_sem).start()

    def take(ref, sem):
        pltpu.make_async_copy(ref, ref, sem).wait()

    tiles = num // 128

    def get_row(stage, row):
        return jnp.concatenate([stage[tile, pl.ds(row, chan, stride=CHUNK), :] for tile in range(tiles)], axis=1)

    def put_row(stage, row, value):
        for tile in range(tiles):
            stage[tile, pl.ds(row, chan, stride=CHUNK), :] = value[:, tile * 128:(tile + 1) * 128]

    def spread(stage, block):
        for tile in range(tiles):
            stage[tile] = block[:, :, tile * 128:(tile + 1) * 128].astype(F32).reshape(chan * CHUNK, 128)

    def gather16(stage, dst):
        for tile in range(tiles):
            dst[:, :, tile * 128:(tile + 1) * 128] = stage[tile].reshape(chan, CHUNK, 128).astype(BF16)

    def input_norm(row):
        z_t = mm_nt(eye[...], z_ref[row])
        return norm_stats(z_t)

    def project(zn_t):
        def piece(blk):
            return mm(w_in_t[blk * chan:(blk + 1) * chan, :], zn_t) + col(blk)
        return piece(0), piece(1), jax.nn.sigmoid(piece(2)), jax.nn.sigmoid(piece(3))

    def mask_of(row):
        return mask_ref[pl.ds(row, 1), :].astype(F32)

    def input_chunk(chunk, carry):
        def one_row(r_in, carry_row):
            row = chunk * CHUNK + r_in
            in_hat, _ = input_norm(row)
            zn_t = (in_hat * col(5) + col(6)).astype(BF16)
            zn_keep[row] = zn_t
            proj_a, proj_b, sig_a, sig_b = project(zn_t)
            mask_f = mask_of(row)
            put_row(stage_a, r_in, mask_f * sig_a * proj_a)
            put_row(stage_b, r_in, mask_f * sig_b * proj_b)
            return carry_row
        lax.fori_loop(0, CHUNK, one_row, 0)
        gather16(stage_b, b_send.at[chunk])
        gather16(stage_a, a_send.at[chunk])

        @pl.when(chunk == 0)
        def _():
            pl.semaphore_wait(barrier, n_dev - 1)

        exchange(lambda peer: b_send.at[chunk, pl.ds(peer * part, part)],
                 b_ch.at[:, pl.ds(me * rows + chunk * CHUNK, CHUNK), :], 0, b_sem)
        exchange(lambda peer: a_send.at[chunk, pl.ds(peer * part, part)],
                 a_ch.at[chunk, :, pl.ds(me * CHUNK, CHUNK), :], 1, a_sem.at[chunk])
        return carry

    lax.fori_loop(0, n_chunk, input_chunk, 0)

    take(b_ch, b_sem)

    def tri_chunk(chunk, carry):
        take(a_ch.at[chunk], a_sem.at[chunk])

        def one(idx, carry_ch):
            o_ch[chunk, idx] = mm_nt(a_ch[chunk, idx], b_ch[idx])
            return carry_ch
        lax.fori_loop(0, part, one, 0)
        exchange(lambda peer: o_ch.at[chunk, :, pl.ds(peer * CHUNK, CHUNK), :],
                 o_row.at[chunk, pl.ds(me * part, part)], 2, o_sem.at[chunk])
        return carry

    lax.fori_loop(0, n_chunk, tri_chunk, 0)

    def chain_chunk(chunk, carry):
        take(o_row.at[chunk], o_sem.at[chunk])
        spread(stage_b, o_row.at[chunk])

        def one_row(r_in, carry_row):
            row = chunk * CHUNK + r_in
            out_hat, out_inv = norm_stats(get_row(stage_b, r_in))
            o_norm = (out_hat * col(7) + col(8)).astype(BF16)
            update = (mm(w_out_t[...], o_norm) + col(9)).astype(BF16).astype(F32)
            zn_t = zn_keep[row]
            sig_g = jax.nn.sigmoid(mm(w_gate_t[...], zn_t) + col(4))
            dy_t = mm_nt(eye[...], dy_ref[row])
            d_update = (sig_g * dy_t).astype(BF16)
            d_gate = dy_t * update * sig_g * (1.0 - sig_g)
            gate16 = d_gate.astype(BF16)
            gg_keep[row] = gate16
            v_acc[4] += lane_fold(d_gate)
            v_acc[9] += lane_fold(d_update.astype(F32))
            m_acc[4 * chan:(4 + 1) * chan, :] += mm_nt(zn_t, gate16)
            m_acc[5 * chan:(5 + 1) * chan, :] += mm_nt(o_norm, d_update)
            d_onorm = mm(w_out_ref[...], d_update).astype(BF16).astype(F32)
            v_acc[7] += lane_fold(d_onorm * out_hat)
            v_acc[8] += lane_fold(d_onorm)
            put_row(stage_a, r_in, norm_back(d_onorm * col(7), out_hat, out_inv))
            return carry_row
        lax.fori_loop(0, CHUNK, one_row, 0)
        gather16(stage_a, do_send.at[chunk])
        exchange(lambda peer: do_send.at[chunk, pl.ds(peer * part, part)],
                 do_ch.at[chunk, :, pl.ds(me * CHUNK, CHUNK), :], 3, do_sem.at[chunk])
        return carry

    lax.fori_loop(0, n_chunk, chain_chunk, 0)

    def da_chunk(chunk, carry):
        take(do_ch.at[chunk], do_sem.at[chunk])

        def one(idx, carry_ch):
            da_ch[chunk, idx] = mm(do_ch[chunk, idx], b_ch[idx]).astype(BF16)
            return carry_ch
        lax.fori_loop(0, part, one, 0)
        exchange(lambda peer: da_ch.at[chunk, :, pl.ds(peer * CHUNK, CHUNK), :],
                 da_row.at[chunk, pl.ds(me * part, part)], 4, da_sem.at[chunk])
        return carry

    lax.fori_loop(0, n_chunk, da_chunk, 0)

    def db_one(idx, carry):
        total = mm_tn(do_ch[0, idx], a_ch[0, idx])
        for chunk in range(1, n_chunk):
            total += mm_tn(do_ch[chunk, idx], a_ch[chunk, idx])
        db_ch[idx] = total.astype(BF16)
        return carry

    lax.fori_loop(0, part, db_one, 0)

    def db_chunk(chunk, carry):
        exchange(lambda peer: db_ch.at[:, pl.ds(peer * rows + chunk * CHUNK, CHUNK), :],
                 db_row.at[chunk, pl.ds(me * part, part)], 5, db_sem.at[chunk])
        return carry

    lax.fori_loop(0, n_chunk, db_chunk, 0)

    def back_chunk(chunk, carry):
        take(da_row.at[chunk], da_sem.at[chunk])
        take(db_row.at[chunk], db_sem.at[chunk])
        spread(stage_a, da_row.at[chunk])
        spread(stage_b, db_row.at[chunk])

        def one_row(r_in, carry_row):
            row = chunk * CHUNK + r_in
            mask_f = mask_of(row)
            zn_t = zn_keep[row]
            proj_a, proj_b, sig_a, sig_b = project(zn_t)
            grad_a = get_row(stage_a, r_in) * mask_f
            grad_b = get_row(stage_b, r_in) * mask_f
            d_znorm = mm(w_gate_ref[...], gg_keep[row])
            pieces = (grad_a * sig_a, grad_b * sig_b,
                      grad_a * proj_a * sig_a * (1.0 - sig_a), grad_b * proj_b * sig_b * (1.0 - sig_b))
            for blk in range(4):
                v_acc[blk] += lane_fold(pieces[blk])
                piece16 = pieces[blk].astype(BF16)
                m_acc[blk * chan:(blk + 1) * chan, :] += mm_nt(zn_t, piece16)
                d_znorm += mm(w_in_ref[:, blk * chan:(blk + 1) * chan], piece16)
            d_znorm = d_znorm.astype(BF16).astype(F32)
            in_hat, in_inv = input_norm(row)
            v_acc[5] += lane_fold(d_znorm * in_hat)
            v_acc[6] += lane_fold(d_znorm)
            dz_t = mm_nt(eye[...], dy_ref[row]) + norm_back(d_znorm * col(5), in_hat, in_inv)
            dz_ref[row] = jnp.transpose(dz_t).astype(BF16)
            return carry_row
        lax.fori_loop(0, CHUNK, one_row, 0)
        return carry

    lax.fori_loop(0, n_chunk, back_chunk, 0)

    v_row[...] = jnp.zeros_like(v_row)
    for idx in range(10):
        v_row[idx:idx + 1, :] = jnp.sum(jnp.transpose(v_acc[idx]), axis=0, keepdims=True)
    exchange(lambda peer: m_acc.at[pl.ds(peer * shard, shard)], m_recv.at[me], 6, m_sem)
    exchange(lambda peer: v_row, v_recv.at[me], 7, v_sem)
    take(m_recv, m_sem)
    g_send[...] = jnp.sum(m_recv[...], axis=0).astype(BF16)
    exchange(lambda peer: g_send, g_all.at[pl.ds(me * shard, shard)], 8, g_sem)
    take(v_recv, v_sem)
    gvec_ref[...] = jnp.sum(v_recv[...], axis=0).astype(BF16)
    take(g_all, g_sem)
    for blk in range(4):
        gw_in_ref[:, blk * chan:(blk + 1) * chan] = g_all[blk * chan:(blk + 1) * chan, :]
    gw_gate_ref[...] = g_all[4 * chan:5 * chan, :]
    gw_out_ref[...] = g_all[5 * chan:6 * chan, :]

    others = (n_dev - 1) * part
    for sent, ref in ((0, b_send), (1, a_send), (3, do_send), (2, o_row), (4, da_row), (5, db_row)):
        take(ref.at[:, pl.ds(0, others)], send_sem.at[sent])
    take(m_recv.at[pl.ds(0, n_dev - 1)], send_sem.at[6])
    take(v_recv.at[pl.ds(0, n_dev - 1)], send_sem.at[7])
    take(g_all.at[pl.ds(0, (n_dev - 1) * shard)], send_sem.at[8])


def local_grads(n_dev, z_loc, mask_loc, dy_loc, ln_in_scale, ln_in_offset, w_in, b_in, ln_out_scale, ln_out_offset, w_out, b_out, w_gate, b_gate):
    rows, num, chan = z_loc.shape
    n_chunk = rows // CHUNK
    part = chan // n_dev
    shard = 6 * chan // n_dev
    vecs = jnp.concatenate([b_in, b_gate, ln_in_scale, ln_in_offset, ln_out_scale, ln_out_offset, b_out]).astype(F32).reshape(10, chan)
    vecs = jnp.pad(vecs, ((0, chan - 10), (0, 0)))
    vmem = pl.BlockSpec(memory_space=pltpu.VMEM)
    shapes = [jax.ShapeDtypeStruct((rows, num, chan), BF16), jax.ShapeDtypeStruct((chan, 4 * chan), BF16),
              jax.ShapeDtypeStruct((chan, chan), BF16), jax.ShapeDtypeStruct((chan, chan), BF16), jax.ShapeDtypeStruct((16, chan), BF16)]
    by_row = pltpu.VMEM((n_chunk, chan, CHUNK, num), BF16)
    by_chan = pltpu.VMEM((n_chunk, part, n_dev * CHUNK, num), BF16)
    by_chan_all = pltpu.VMEM((part, num, num), BF16)
    stage = pltpu.VMEM((num // 128, chan * CHUNK, 128), F32)
    keep = pltpu.VMEM((rows, chan, num), BF16)
    scratch = [
        pltpu.VMEM((4 * chan, chan), BF16), pltpu.VMEM((chan, chan), BF16), pltpu.VMEM((chan, chan), BF16), pltpu.VMEM((chan, chan), BF16),
        pltpu.VMEM((chan, chan), F32),
        by_row, by_row, by_chan, by_chan_all,
        pltpu.VMEM((n_chunk, part, n_dev * CHUNK, num), F32), pltpu.VMEM((n_chunk, chan, CHUNK, num), F32),
        by_row, by_chan, by_chan, by_row, by_chan_all, by_row,
        stage, stage, keep, keep,
        pltpu.VMEM((6 * chan, chan), F32), pltpu.VMEM((10, chan, chan), F32), pltpu.VMEM((16, chan), F32),
        pltpu.VMEM((n_dev, shard, chan), F32), pltpu.VMEM((n_dev, 16, chan), F32),
        pltpu.VMEM((shard, chan), BF16), pltpu.VMEM((6 * chan, chan), BF16),
        pltpu.SemaphoreType.DMA((9,)),
        pltpu.SemaphoreType.DMA((n_chunk,)), pltpu.SemaphoreType.DMA, pltpu.SemaphoreType.DMA((n_chunk,)),
        pltpu.SemaphoreType.DMA((n_chunk,)), pltpu.SemaphoreType.DMA((n_chunk,)), pltpu.SemaphoreType.DMA((n_chunk,)),
        pltpu.SemaphoreType.DMA, pltpu.SemaphoreType.DMA, pltpu.SemaphoreType.DMA,
    ]
    d_z, gw_in, gw_gate, gw_out, gvec = pl.pallas_call(
        functools.partial(kernel, n_dev),
        out_shape=shapes,
        in_specs=[vmem] * 7,
        out_specs=[vmem] * 5,
        scratch_shapes=scratch,
        compiler_params=pltpu.CompilerParams(collective_id=0, has_side_effects=True, vmem_limit_bytes=66 * 1024 * 1000),
        name='triangle_backward',
    )(z_loc, dy_loc, mask_loc, w_in, w_gate, w_out, vecs)
    d_b_in = gvec[:4].reshape(4 * chan)
    return (d_z, gvec[5], gvec[6], gw_in, d_b_in, gvec[7], gvec[8], gw_out, gvec[9], gw_gate, gvec[4])


def solution(mesh):
    n_dev = mesh.shape['dap']
    pair_spec = P(('batch', 'dap'), None, None)
    mask_spec = P(('batch', 'dap'), None)
    vec_rep = P(None)
    mat_rep = P(None, None)
    vec_part = P('batch')
    mat_part = P('batch', None)
    in_specs = (pair_spec, mask_spec, pair_spec, vec_rep, vec_rep, mat_rep, vec_rep, vec_rep, vec_rep, mat_rep, vec_rep, mat_rep, vec_rep)
    out_specs = (pair_spec, vec_part, vec_part, mat_part, vec_part, vec_part, vec_part, mat_part, vec_part, mat_part, vec_part)
    return jax.shard_map(functools.partial(local_grads, n_dev), mesh=mesh, in_specs=in_specs, out_specs=out_specs, check_vma=False)
```

```python
import functools
import jax
import jax.numpy as jnp
from jax import lax
from jax.experimental import pallas as pl
from jax.experimental.pallas import tpu as pltpu
from jax.sharding import PartitionSpec as P

LN_EPS = 1e-5
CHUNK = 8
F32 = jnp.float32
BF16 = jnp.bfloat16


def mm(x_val, y_val):
    return lax.dot_general(x_val, y_val, (((1,), (0,)), ((), ())), preferred_element_type=F32)


def mm_nt(x_val, y_val):
    return lax.dot_general(x_val, y_val, (((1,), (1,)), ((), ())), preferred_element_type=F32)


def mm_tn(x_val, y_val):
    return lax.dot_general(x_val, y_val, (((0,), (0,)), ((), ())), preferred_element_type=F32)


def norm_stats(x_val):
    size = x_val.shape[0]
    mean_val = jnp.sum(x_val, axis=0, keepdims=True) * (1.0 / size)
    centered = x_val - mean_val
    inv_std = lax.rsqrt(jnp.sum(centered * centered, axis=0, keepdims=True) * (1.0 / size) + LN_EPS)
    return centered * inv_std, inv_std


def norm_back(grad_hat, x_hat, inv_std):
    size = x_hat.shape[0]
    mean_grad = jnp.sum(grad_hat, axis=0, keepdims=True) * (1.0 / size)
    mean_proj = jnp.sum(grad_hat * x_hat, axis=0, keepdims=True) * (1.0 / size)
    return inv_std * (grad_hat - mean_grad - x_hat * mean_proj)


def lane_fold(x_val):
    total = x_val[:, :128]
    for tile in range(1, x_val.shape[1] // 128):
        total = total + x_val[:, tile * 128:(tile + 1) * 128]
    return total


def kernel(n_dev, z_hbm, dy_hbm, mask_ref, w_in_ref, w_gate_ref, w_out_ref, *refs):
    par_refs = refs[:7]
    (dz_hbm, gmat_ref, gvec_ref,
     z_ref, dy_ref, dz_ref, w_in_t, w_gate_t, w_out_t, eye, par, cols,
     a_send, b_send, a_ch, b_ch, o_ch, o_row, do_send, do_ch, da_ch, da_row, db_ch, db_row,
     stage_a, stage_b, zn_keep, gg_keep, dzn_keep, m_acc, v_acc, v_row, m_recv, v_recv, g_send, g_all,
     z_sem, dy_sem, dz_sem, send_sem, a_sem, b_sem, o_sem, do_sem, da_sem, db_sem, m_sem, v_sem, g_sem) = refs[7:]
    rows, num, chan = z_ref.shape
    n_chunk = rows // CHUNK
    part = chan // n_dev
    tiles = num // 128
    me = lax.axis_index('dap')
    shard = g_send.shape[1]
    band = shard * n_dev

    barrier = pltpu.get_barrier_semaphore()

    def ring_peer(step):
        half = step // 2 + 1
        offset = half + lax.rem(step, 2) * (n_dev - 2 * half)
        return lax.rem(me + offset, n_dev)

    def hello(step, carry):
        pl.semaphore_signal(barrier, inc=1, device_id={'dap': ring_peer(step)}, device_id_type=pl.DeviceIdType.MESH)
        return carry

    lax.fori_loop(0, n_dev - 1, hello, 0)

    def block(chunk):
        return pl.ds(chunk * CHUNK, CHUNK)

    def load_z(chunk):
        return pltpu.make_async_copy(z_hbm.at[block(chunk)], z_ref.at[block(chunk)], z_sem.at[chunk])

    def load_dy():
        return pltpu.make_async_copy(dy_hbm, dy_ref, dy_sem)

    def store_dz(chunk):
        return pltpu.make_async_copy(dz_ref.at[block(chunk)], dz_hbm.at[block(chunk)], dz_sem.at[chunk])

    for chunk in range(n_chunk):
        load_z(chunk).start()
    load_dy().start()

    row_id = lax.broadcasted_iota(jnp.int32, (chan, chan), 0)
    col_id = lax.broadcasted_iota(jnp.int32, (chan, chan), 1)
    eye[...] = jnp.where(row_id == col_id, 1.0, 0.0).astype(BF16)
    par[...] = jnp.zeros_like(par)
    top = 0
    for ref in par_refs:
        par[top:top + ref.shape[0], :] = ref[...].astype(F32)
        top += ref.shape[0]
    cols[...] = jnp.transpose(par[...])
    for blk in range(4):
        w_in_t[blk * chan:(blk + 1) * chan, :] = jnp.transpose(w_in_ref[:, blk * chan:(blk + 1) * chan].astype(F32)).astype(BF16)
    w_gate_t[...] = jnp.transpose(w_gate_ref[...].astype(F32)).astype(BF16)
    w_out_t[...] = jnp.transpose(w_out_ref[...].astype(F32)).astype(BF16)
    m_acc[...] = jnp.zeros_like(m_acc)
    v_acc[...] = jnp.zeros_like(v_acc)
    v_row[...] = jnp.zeros_like(v_row)

    def col(idx):
        return cols[:, idx:idx + 1]

    def exchange(src_of, dst_ref, send_idx, recv_sem):
        def one(step, carry):
            peer = ring_peer(step)
            pltpu.make_async_remote_copy(
                src_ref=src_of(peer), dst_ref=dst_ref, send_sem=send_sem.at[send_idx], recv_sem=recv_sem,
                device_id={'dap': peer}, device_id_type=pl.DeviceIdType.MESH).start()
            return carry
        lax.fori_loop(0, n_dev - 1, one, 0)
        pltpu.make_async_copy(src_of(me), dst_ref, recv_sem).start()

    def take(ref, sem):
        pltpu.make_async_copy(ref, ref, sem).wait()

    def lanes(span, tile):
        return slice((span[0] + tile) * 128, (span[0] + tile + 1) * 128)

    def whole(span):
        return slice(span[0] * 128, span[1] * 128)

    def get_row(stage, row, span):
        return jnp.concatenate([stage[tile, pl.ds(row, chan, stride=CHUNK), :] for tile in range(*span)], axis=1)

    def put_row(stage, row, value, span):
        for tile in range(span[1] - span[0]):
            stage[span[0] + tile, pl.ds(row, chan, stride=CHUNK), :] = value[:, tile * 128:(tile + 1) * 128]

    def spread(stage, src, span):
        for tile in range(*span):
            stage[tile] = src[:, :, tile * 128:(tile + 1) * 128].astype(F32).reshape(chan * CHUNK, 128)

    def gather16(stage, dst, span):
        for tile in range(*span):
            dst[:, :, tile * 128:(tile + 1) * 128] = stage[tile].reshape(chan, CHUNK, 128).astype(BF16)

    everything = (0, tiles)

    def input_norm(row, span):
        z_t = mm_nt(eye[...], z_ref[row, whole(span), :])
        return norm_stats(z_t)

    def piece_of(blk, zn_t):
        return mm(w_in_t[blk * chan:(blk + 1) * chan, :], zn_t) + col(blk)

    def mask_of(row, span):
        return mask_ref[pl.ds(row, 1), :].astype(F32)[:, whole(span)]

    def input_piece(chunk, span):
        def one_row(r_in, carry_row):
            row = chunk * CHUNK + r_in
            in_hat, _ = input_norm(row, span)
            zn_t = (in_hat * col(5) + col(6)).astype(BF16)
            zn_keep[row, :, whole(span)] = zn_t
            mask_f = mask_of(row, span)
            put_row(stage_a, r_in, mask_f * jax.nn.sigmoid(piece_of(2, zn_t)) * piece_of(0, zn_t), span)
            put_row(stage_b, r_in, mask_f * jax.nn.sigmoid(piece_of(3, zn_t)) * piece_of(1, zn_t), span)
            return carry_row
        lax.fori_loop(0, CHUNK, one_row, 0)
        gather16(stage_b, b_send.at[chunk], span)
        gather16(stage_a, a_send.at[chunk], span)

    def input_send(chunk, span):
        exchange(lambda peer: b_send.at[chunk, pl.ds(peer * part, part), :, whole(span)],
                 b_ch.at[:, pl.ds(me * rows + chunk * CHUNK, CHUNK), whole(span)], 0, b_sem)
        exchange(lambda peer: a_send.at[chunk, pl.ds(peer * part, part), :, whole(span)],
                 a_ch.at[chunk, :, pl.ds(me * CHUNK, CHUNK), whole(span)], 1, a_sem.at[chunk])

    load_z(0).wait()
    for tile in range(tiles):
        input_piece(0, (tile, tile + 1))
        if tile == 0:
            pl.semaphore_wait(barrier, n_dev - 1)
        input_send(0, (tile, tile + 1))

    def input_chunk(chunk, carry):
        load_z(chunk).wait()
        input_piece(chunk, everything)
        input_send(chunk, everything)
        return carry

    lax.fori_loop(1, n_chunk, input_chunk, 0)

    take(b_ch, b_sem)

    def tri_chunk(chunk, carry):
        take(a_ch.at[chunk], a_sem.at[chunk])

        def one(idx, carry_ch):
            o_ch[chunk, idx] = mm_nt(a_ch[chunk, idx], b_ch[idx])
            return carry_ch
        lax.fori_loop(0, part, one, 0)
        exchange(lambda peer: o_ch.at[chunk, :, pl.ds(peer * CHUNK, CHUNK), :],
                 o_row.at[chunk, pl.ds(me * part, part)], 2, o_sem.at[chunk])
        return carry

    lax.fori_loop(0, n_chunk, tri_chunk, 0)
    load_dy().wait()

    def grow(blk, value):
        m_acc[blk * chan:(blk + 1) * chan, :] += value

    def chain_chunk(chunk, carry):
        take(o_row.at[chunk], o_sem.at[chunk])
        spread(stage_b, o_row.at[chunk], everything)

        def one_row(r_in, carry_row):
            row = chunk * CHUNK + r_in
            out_hat, out_inv = norm_stats(get_row(stage_b, r_in, everything))
            o_norm = (out_hat * col(7) + col(8)).astype(BF16)
            update = (mm(w_out_t[...], o_norm) + col(9)).astype(BF16).astype(F32)
            zn_t = zn_keep[row]
            sig_g = jax.nn.sigmoid(mm(w_gate_t[...], zn_t) + col(4))
            dy_t = mm_nt(eye[...], dy_ref[row])
            d_update = (sig_g * dy_t).astype(BF16)
            d_gate = dy_t * update * sig_g * (1.0 - sig_g)
            gate16 = d_gate.astype(BF16)
            gg_keep[row] = gate16
            v_acc[0] += lane_fold(d_gate)
            v_acc[1] += lane_fold(d_update.astype(F32))
            grow(0, mm_nt(zn_t, gate16))
            grow(1, mm_nt(o_norm, d_update))
            d_onorm = mm(w_out_ref[...], d_update).astype(BF16).astype(F32)
            v_acc[2] += lane_fold(d_onorm * out_hat)
            v_acc[3] += lane_fold(d_onorm)
            put_row(stage_a, r_in, norm_back(d_onorm * col(7), out_hat, out_inv), everything)
            return carry_row
        lax.fori_loop(0, CHUNK, one_row, 0)
        gather16(stage_a, do_send.at[chunk], everything)
        exchange(lambda peer: do_send.at[chunk, pl.ds(peer * part, part)],
                 do_ch.at[chunk, :, pl.ds(me * CHUNK, CHUNK), :], 3, do_sem.at[chunk])
        return carry

    lax.fori_loop(0, n_chunk, chain_chunk, 0)

    def share_out(turn, kinds):
        for pos, kind in enumerate(kinds):
            v_row[turn, pos:pos + 1, :] = jnp.sum(jnp.transpose(v_acc[kind]), axis=0, keepdims=True)
        exchange(lambda peer: m_acc.at[pl.ds(turn * band + peer * shard, shard)], m_recv.at[turn, me], 6, m_sem.at[turn])
        exchange(lambda peer: v_row.at[turn], v_recv.at[turn, me], 7, v_sem.at[turn])

    def share_sum(turn):
        take(m_recv.at[turn], m_sem.at[turn])
        g_send[turn] = jnp.sum(m_recv[turn], axis=0).astype(BF16)
        exchange(lambda peer: g_send.at[turn], g_all.at[pl.ds(turn * band + me * shard, shard)], 8, g_sem)
        take(v_recv.at[turn], v_sem.at[turn])
        gvec_ref[turn] = jnp.sum(v_recv[turn], axis=0).astype(BF16)

    share_out(0, (0, 1, 2, 3))

    def da_chunk(chunk, carry):
        take(do_ch.at[chunk], do_sem.at[chunk])

        def one(idx, carry_ch):
            da_ch[chunk, idx] = mm(do_ch[chunk, idx], b_ch[idx]).astype(BF16)
            return carry_ch
        lax.fori_loop(0, part, one, 0)
        exchange(lambda peer: da_ch.at[chunk, :, pl.ds(peer * CHUNK, CHUNK), :],
                 da_row.at[chunk, pl.ds(me * part, part)], 4, da_sem.at[chunk])
        return carry

    lax.fori_loop(0, n_chunk, da_chunk, 0)

    def db_one(idx, carry):
        total = mm_tn(do_ch[0, idx], a_ch[0, idx])
        for chunk in range(1, n_chunk):
            total += mm_tn(do_ch[chunk, idx], a_ch[chunk, idx])
        db_ch[idx] = total.astype(BF16)
        return carry

    lax.fori_loop(0, part, db_one, 0)

    def db_send(chunk, span, sem):
        exchange(lambda peer: db_ch.at[:, pl.ds(peer * rows + chunk * CHUNK, CHUNK), whole(span)],
                 db_row.at[chunk, pl.ds(me * part, part), :, whole(span)], 5, sem)

    last = n_chunk - 1
    for chunk in range(last):
        db_send(chunk, everything, db_sem.at[chunk])
    for tile in range(tiles):
        db_send(last, (tile, tile + 1), db_sem.at[last + tile])
    share_sum(0)

    def half_back(row, r_in, stage, blk, zn_t, span):
        grad = get_row(stage, r_in, span) * mask_of(row, span)
        proj = piece_of(blk, zn_t)
        sig = jax.nn.sigmoid(piece_of(blk + 2, zn_t))
        d_proj = grad * sig
        d_sig = d_proj * proj * (1.0 - sig)
        grow(2 + 2 * blk, mm_nt(zn_t, d_proj.astype(BF16)))
        grow(3 + 2 * blk, mm_nt(zn_t, d_sig.astype(BF16)))
        v_acc[4 + 2 * blk] += lane_fold(d_proj)
        v_acc[5 + 2 * blk] += lane_fold(d_sig)
        return (mm(w_in_ref[:, blk * chan:(blk + 1) * chan], d_proj.astype(BF16))
                + mm(w_in_ref[:, (blk + 2) * chan:(blk + 3) * chan], d_sig.astype(BF16)))

    def early_chunk(chunk, carry):
        take(da_row.at[chunk], da_sem.at[chunk])
        spread(stage_a, da_row.at[chunk], everything)

        def one_row(r_in, carry_row):
            row = chunk * CHUNK + r_in
            dzn_keep[row] = mm(w_gate_ref[...], gg_keep[row]) + half_back(row, r_in, stage_a, 0, zn_keep[row], everything)
            return carry_row
        lax.fori_loop(0, CHUNK, one_row, 0)
        return carry

    lax.fori_loop(0, n_chunk, early_chunk, 0)
    share_out(1, (4, 5))

    def late_piece(chunk, span):
        spread(stage_b, db_row.at[chunk], span)

        def one_row(r_in, carry_row):
            row = chunk * CHUNK + r_in
            zn_t = zn_keep[row, :, whole(span)]
            d_znorm = (dzn_keep[row, :, whole(span)] + half_back(row, r_in, stage_b, 1, zn_t, span)).astype(BF16).astype(F32)
            in_hat, in_inv = input_norm(row, span)
            v_acc[8] += lane_fold(d_znorm * in_hat)
            v_acc[9] += lane_fold(d_znorm)
            dz_t = mm_nt(eye[...], dy_ref[row, whole(span), :]) + norm_back(d_znorm * col(5), in_hat, in_inv)
            dz_ref[row, whole(span), :] = jnp.transpose(dz_t).astype(BF16)
            return carry_row
        lax.fori_loop(0, CHUNK, one_row, 0)

    def late_chunk(chunk, carry):
        take(db_row.at[chunk], db_sem.at[chunk])
        late_piece(chunk, everything)
        store_dz(chunk).start()
        return carry

    lax.fori_loop(0, last, late_chunk, 0)
    for tile in range(tiles):
        span = (tile, tile + 1)
        take(db_row.at[last, :, :, whole(span)], db_sem.at[last + tile])
        late_piece(last, span)
    share_out(2, (6, 7, 8, 9))
    store_dz(last).start()
    share_sum(1)
    share_sum(2)
    take(g_all, g_sem)
    for pos, blk in enumerate((4, 5, 0, 2, 1, 3)):
        gmat_ref[:, blk * chan:(blk + 1) * chan] = g_all[pos * chan:(pos + 1) * chan, :]

    others = (n_dev - 1) * part
    for sent, ref in ((0, b_send), (1, a_send), (3, do_send), (2, o_row), (4, da_row), (5, db_row)):
        take(ref.at[:, pl.ds(0, others)], send_sem.at[sent])
    take(m_recv.at[:, pl.ds(0, n_dev - 1)], send_sem.at[6])
    take(v_recv.at[:, pl.ds(0, n_dev - 1)], send_sem.at[7])
    take(g_all.at[pl.ds(0, 3 * (n_dev - 1) * shard)], send_sem.at[8])
    for chunk in range(n_chunk):
        store_dz(chunk).wait()


def local_grads(n_dev, z_loc, mask_loc, dy_loc, ln_in_scale, ln_in_offset, w_in, b_in, ln_out_scale, ln_out_offset, w_out, b_out, w_gate, b_gate):
    rows, num, chan = z_loc.shape
    n_chunk = rows // CHUNK
    part = chan // n_dev
    tiles = num // 128
    shard = 2 * chan // n_dev
    params = [vec.reshape(-1, chan) for vec in (b_in, b_gate, ln_in_scale, ln_in_offset, ln_out_scale, ln_out_offset, b_out)]
    vmem = pl.BlockSpec(memory_space=pltpu.VMEM)
    hbm = pl.BlockSpec(memory_space=pl.ANY)
    shapes = [jax.ShapeDtypeStruct((rows, num, chan), BF16), jax.ShapeDtypeStruct((chan, 6 * chan), BF16), jax.ShapeDtypeStruct((3, 8, chan), BF16)]
    pair = pltpu.VMEM((rows, num, chan), BF16)
    by_row = pltpu.VMEM((n_chunk, chan, CHUNK, num), BF16)
    by_chan = pltpu.VMEM((n_chunk, part, n_dev * CHUNK, num), BF16)
    by_chan_all = pltpu.VMEM((part, num, num), BF16)
    stage = pltpu.VMEM((tiles, chan * CHUNK, 128), F32)
    keep = pltpu.VMEM((rows, chan, num), BF16)
    square = pltpu.VMEM((chan, chan), BF16)
    dma = pltpu.SemaphoreType.DMA
    scratch = [
        pair, pair, pair, pltpu.VMEM((4 * chan, chan), BF16), square, square, square,
        pltpu.VMEM((chan, chan), F32), pltpu.VMEM((chan, chan), F32),
        by_row, by_row, by_chan, by_chan_all,
        pltpu.VMEM((n_chunk, part, n_dev * CHUNK, num), F32), pltpu.VMEM((n_chunk, chan, CHUNK, num), F32),
        by_row, by_chan, by_chan, by_row, by_chan_all, by_row,
        stage, stage, keep, keep, pltpu.VMEM((rows, chan, num), F32),
        pltpu.VMEM((6 * chan, chan), F32), pltpu.VMEM((10, chan, chan), F32), pltpu.VMEM((3, 8, chan), F32),
        pltpu.VMEM((3, n_dev, shard, chan), F32), pltpu.VMEM((3, n_dev, 8, chan), F32),
        pltpu.VMEM((3, shard, chan), BF16), pltpu.VMEM((6 * chan, chan), BF16),
        dma((n_chunk,)), dma, dma((n_chunk,)), dma((9,)),
        dma((n_chunk,)), dma, dma((n_chunk,)), dma((n_chunk,)), dma((n_chunk,)), dma((n_chunk - 1 + tiles,)),
        dma((3,)), dma((3,)), dma,
    ]
    d_z, gmat, gvec = pl.pallas_call(
        functools.partial(kernel, n_dev),
        out_shape=shapes,
        in_specs=[hbm, hbm] + [vmem] * 11,
        out_specs=[hbm, vmem, vmem],
        scratch_shapes=scratch,
        compiler_params=pltpu.CompilerParams(collective_id=0, has_side_effects=True, vmem_limit_bytes=67000000),
        name='triangle_backward',
    )(z_loc, dy_loc, mask_loc, w_in, w_gate, w_out, *params)
    d_b_in = jnp.concatenate([gvec[1, 0], gvec[2, 0], gvec[1, 1], gvec[2, 1]])
    return (d_z, gvec[2, 2], gvec[2, 3], gmat[:, :4 * chan], d_b_in, gvec[0, 2], gvec[0, 3],
            gmat[:, 5 * chan:], gvec[0, 1], gmat[:, 4 * chan:5 * chan], gvec[0, 0])


def solution(mesh):
    n_dev = mesh.shape['dap']
    pair_spec = P(('batch', 'dap'), None, None)
    mask_spec = P(('batch', 'dap'), None)
    vec_rep = P(None)
    mat_rep = P(None, None)
    vec_part = P('batch')
    mat_part = P('batch', None)
    in_specs = (pair_spec, mask_spec, pair_spec, vec_rep, vec_rep, mat_rep, vec_rep, vec_rep, vec_rep, mat_rep, vec_rep, mat_rep, vec_rep)
    out_specs = (pair_spec, vec_part, vec_part, mat_part, vec_part, vec_part, vec_part, mat_part, vec_part, mat_part, vec_part)
    return jax.shard_map(functools.partial(local_grads, n_dev), mesh=mesh, in_specs=in_specs, out_specs=out_specs, check_vma=False)
```

```python
import functools
import jax
import jax.numpy as jnp
from jax import lax
from jax.experimental import pallas as pl
from jax.experimental.pallas import tpu as pltpu
from jax.sharding import PartitionSpec as P

LN_EPS = 1e-5
CHUNK = 8
F32 = jnp.float32
BF16 = jnp.bfloat16


def mm(x_val, y_val):
    return lax.dot_general(x_val, y_val, (((1,), (0,)), ((), ())), preferred_element_type=F32)


def mm_nt(x_val, y_val):
    return lax.dot_general(x_val, y_val, (((1,), (1,)), ((), ())), preferred_element_type=F32)


def mm_tn(x_val, y_val):
    return lax.dot_general(x_val, y_val, (((0,), (0,)), ((), ())), preferred_element_type=F32)


def norm_stats(x_val):
    size = x_val.shape[0]
    mean_val = jnp.sum(x_val, axis=0, keepdims=True) * (1.0 / size)
    centered = x_val - mean_val
    inv_std = lax.rsqrt(jnp.sum(centered * centered, axis=0, keepdims=True) * (1.0 / size) + LN_EPS)
    return centered * inv_std, inv_std


def norm_back(grad_hat, x_hat, inv_std):
    size = x_hat.shape[0]
    mean_grad = jnp.sum(grad_hat, axis=0, keepdims=True) * (1.0 / size)
    mean_proj = jnp.sum(grad_hat * x_hat, axis=0, keepdims=True) * (1.0 / size)
    return inv_std * (grad_hat - mean_grad - x_hat * mean_proj)


def lane_fold(x_val):
    total = x_val[:, :128]
    for tile in range(1, x_val.shape[1] // 128):
        total = total + x_val[:, tile * 128:(tile + 1) * 128]
    return total


def kernel(n_dev, z_hbm, dy_hbm, mask_ref, w_in_ref, w_gate_ref, w_out_ref, *refs):
    par_refs = refs[:7]
    (dz_hbm, gmat_ref, gvec_ref,
     z_ref, dy_ref, dz_ref, w_in_t, w_gate_t, w_out_t, eye, par, cols,
     a_send, b_send, a_ch, b_ch, o_ch, o_row, do_send, do_ch, da_ch, da_row, db_ch, db_row,
     stage_a, stage_b, zn_keep, gg_keep, dzn_keep, m_acc, v_acc, v_row, m_recv, v_recv, g_send, g_all,
     z_sem, dy_sem, dz_sem, send_sem, a_sem, b_sem, o_sem, do_sem, da_sem, db_sem, m_sem, v_sem, g_sem) = refs[7:]
    rows, num, chan = z_ref.shape
    n_chunk = rows // CHUNK
    part = chan // n_dev
    tiles = num // 128
    me = lax.axis_index('dap')
    shard = g_send.shape[1]
    band = shard * n_dev

    barrier = pltpu.get_barrier_semaphore()

    def ring_peer(step):
        half = step // 2 + 1
        offset = half + lax.rem(step, 2) * (n_dev - 2 * half)
        return lax.rem(me + offset, n_dev)

    def hello(step, carry):
        pl.semaphore_signal(barrier, inc=1, device_id={'dap': ring_peer(step)}, device_id_type=pl.DeviceIdType.MESH)
        return carry

    lax.fori_loop(0, n_dev - 1, hello, 0)

    def block(chunk):
        return pl.ds(chunk * CHUNK, CHUNK)

    def load_z(chunk):
        return pltpu.make_async_copy(z_hbm.at[block(chunk)], z_ref.at[block(chunk)], z_sem.at[chunk])

    def load_dy():
        return pltpu.make_async_copy(dy_hbm, dy_ref, dy_sem)

    def store_dz(chunk):
        return pltpu.make_async_copy(dz_ref.at[block(chunk)], dz_hbm.at[block(chunk)], dz_sem.at[chunk])

    for chunk in range(n_chunk):
        load_z(chunk).start()
    load_dy().start()

    row_id = lax.broadcasted_iota(jnp.int32, (chan, chan), 0)
    col_id = lax.broadcasted_iota(jnp.int32, (chan, chan), 1)
    eye[...] = jnp.where(row_id == col_id, 1.0, 0.0).astype(BF16)
    par[...] = jnp.zeros_like(par)
    top = 0
    for ref in par_refs:
        par[top:top + ref.shape[0], :] = ref[...].astype(F32)
        top += ref.shape[0]
    cols[...] = jnp.transpose(par[...])
    for blk in range(4):
        w_in_t[blk * chan:(blk + 1) * chan, :] = jnp.transpose(w_in_ref[:, blk * chan:(blk + 1) * chan].astype(F32)).astype(BF16)
    w_gate_t[...] = jnp.transpose(w_gate_ref[...].astype(F32)).astype(BF16)
    w_out_t[...] = jnp.transpose(w_out_ref[...].astype(F32)).astype(BF16)
    m_acc[...] = jnp.zeros_like(m_acc)
    v_acc[...] = jnp.zeros_like(v_acc)
    v_row[...] = jnp.zeros_like(v_row)

    def col(idx):
        return cols[:, idx:idx + 1]

    def exchange(src_of, dst_ref, send_idx, recv_sem):
        def one(step, carry):
            peer = ring_peer(step)
            pltpu.make_async_remote_copy(
                src_ref=src_of(peer), dst_ref=dst_ref, send_sem=send_sem.at[send_idx], recv_sem=recv_sem,
                device_id={'dap': peer}, device_id_type=pl.DeviceIdType.MESH).start()
            return carry
        lax.fori_loop(0, n_dev - 1, one, 0)
        pltpu.make_async_copy(src_of(me), dst_ref, recv_sem).start()

    def take(ref, sem):
        pltpu.make_async_copy(ref, ref, sem).wait()

    def lanes(span, tile):
        return slice((span[0] + tile) * 128, (span[0] + tile + 1) * 128)

    def whole(span):
        return slice(span[0] * 128, span[1] * 128)

    def get_row(stage, row, span):
        return jnp.concatenate([stage[tile, pl.ds(row, chan, stride=CHUNK), :] for tile in range(*span)], axis=1)

    def put_row(stage, row, value, span):
        for tile in range(span[1] - span[0]):
            stage[span[0] + tile, pl.ds(row, chan, stride=CHUNK), :] = value[:, tile * 128:(tile + 1) * 128]

    def spread(stage, src, span):
        for tile in range(*span):
            stage[tile] = src[:, :, tile * 128:(tile + 1) * 128].astype(F32).reshape(chan * CHUNK, 128)

    def gather16(stage, dst, span):
        for tile in range(*span):
            dst[:, :, tile * 128:(tile + 1) * 128] = stage[tile].reshape(chan, CHUNK, 128).astype(BF16)

    everything = (0, tiles)

    def input_norm(row, span):
        z_t = mm_nt(eye[...], z_ref[row, whole(span), :])
        return norm_stats(z_t)

    def piece_of(blk, zn_t):
        return mm(w_in_t[blk * chan:(blk + 1) * chan, :], zn_t) + col(blk)

    def mask_of(row, span):
        return mask_ref[pl.ds(row, 1), :].astype(F32)[:, whole(span)]

    def input_piece(chunk, span):
        def one_row(r_in, carry_row):
            row = chunk * CHUNK + r_in
            in_hat, _ = input_norm(row, span)
            zn_t = (in_hat * col(5) + col(6)).astype(BF16)
            zn_keep[row, :, whole(span)] = zn_t
            mask_f = mask_of(row, span)
            put_row(stage_a, r_in, mask_f * jax.nn.sigmoid(piece_of(2, zn_t)) * piece_of(0, zn_t), span)
            put_row(stage_b, r_in, mask_f * jax.nn.sigmoid(piece_of(3, zn_t)) * piece_of(1, zn_t), span)
            return carry_row
        lax.fori_loop(0, CHUNK, one_row, 0)
        gather16(stage_b, b_send.at[chunk], span)
        gather16(stage_a, a_send.at[chunk], span)

    def input_send(chunk, span):
        exchange(lambda peer: b_send.at[chunk, pl.ds(peer * part, part), :, whole(span)],
                 b_ch.at[:, pl.ds(me * rows + chunk * CHUNK, CHUNK), whole(span)], 0, b_sem)
        exchange(lambda peer: a_send.at[chunk, pl.ds(peer * part, part), :, whole(span)],
                 a_ch.at[chunk, :, pl.ds(me * CHUNK, CHUNK), whole(span)], 1, a_sem.at[chunk])

    load_z(0).wait()
    for tile in range(tiles):
        input_piece(0, (tile, tile + 1))
        if tile == 0:
            pl.semaphore_wait(barrier, n_dev - 1)
        input_send(0, (tile, tile + 1))

    def input_chunk(chunk, carry):
        load_z(chunk).wait()
        input_piece(chunk, everything)
        input_send(chunk, everything)
        return carry

    lax.fori_loop(1, n_chunk, input_chunk, 0)

    take(b_ch, b_sem)

    def tri_chunk(chunk, carry):
        take(a_ch.at[chunk], a_sem.at[chunk])

        def one(idx, carry_ch):
            o_ch[chunk, idx] = mm_nt(a_ch[chunk, idx], b_ch[idx])
            return carry_ch
        lax.fori_loop(0, part, one, 0)
        exchange(lambda peer: o_ch.at[chunk, :, pl.ds(peer * CHUNK, CHUNK), :],
                 o_row.at[chunk, pl.ds(me * part, part)], 2, o_sem.at[chunk])
        return carry

    lax.fori_loop(0, n_chunk, tri_chunk, 0)
    load_dy().wait()

    def grow(blk, value):
        m_acc[blk * chan:(blk + 1) * chan, :] += value

    def chain_chunk(chunk, carry):
        take(o_row.at[chunk], o_sem.at[chunk])
        spread(stage_b, o_row.at[chunk], everything)

        def one_row(r_in, carry_row):
            row = chunk * CHUNK + r_in
            out_hat, out_inv = norm_stats(get_row(stage_b, r_in, everything))
            o_norm = (out_hat * col(7) + col(8)).astype(BF16)
            update = (mm(w_out_t[...], o_norm) + col(9)).astype(BF16).astype(F32)
            zn_t = zn_keep[row]
            sig_g = jax.nn.sigmoid(mm(w_gate_t[...], zn_t) + col(4))
            dy_t = mm_nt(eye[...], dy_ref[row])
            d_update = (sig_g * dy_t).astype(BF16)
            d_gate = dy_t * update * sig_g * (1.0 - sig_g)
            gate16 = d_gate.astype(BF16)
            gg_keep[row] = gate16
            v_acc[0] += lane_fold(d_gate)
            v_acc[1] += lane_fold(d_update.astype(F32))
            grow(0, mm_nt(zn_t, gate16))
            grow(1, mm_nt(o_norm, d_update))
            d_onorm = mm(w_out_ref[...], d_update).astype(BF16).astype(F32)
            v_acc[2] += lane_fold(d_onorm * out_hat)
            v_acc[3] += lane_fold(d_onorm)
            put_row(stage_a, r_in, norm_back(d_onorm * col(7), out_hat, out_inv), everything)
            return carry_row
        lax.fori_loop(0, CHUNK, one_row, 0)
        gather16(stage_a, do_send.at[chunk], everything)
        exchange(lambda peer: do_send.at[chunk, pl.ds(peer * part, part)],
                 do_ch.at[chunk, :, pl.ds(me * CHUNK, CHUNK), :], 3, do_sem.at[chunk])
        return carry

    lax.fori_loop(0, n_chunk, chain_chunk, 0)

    def share_out(turn, kinds):
        exchange(lambda peer: m_acc.at[pl.ds(turn * band + peer * shard, shard)], m_recv.at[turn, me], 6, m_sem.at[turn])
        if kinds:
            for pos, kind in enumerate(kinds):
                v_row[turn - 1, pos:pos + 1, :] = jnp.sum(jnp.transpose(v_acc[kind]), axis=0, keepdims=True)
            exchange(lambda peer: v_row.at[turn - 1], v_recv.at[turn - 1, me], 7, v_sem.at[turn - 1])

    def share_sum(turn):
        take(m_recv.at[turn], m_sem.at[turn])
        g_send[turn] = jnp.sum(m_recv[turn], axis=0).astype(BF16)
        exchange(lambda peer: g_send.at[turn], g_all.at[pl.ds(turn * band + me * shard, shard)], 8, g_sem)
        if turn:
            take(v_recv.at[turn - 1], v_sem.at[turn - 1])
            gvec_ref[turn - 1] = jnp.sum(v_recv[turn - 1], axis=0).astype(BF16)

    share_out(0, ())

    def da_chunk(chunk, carry):
        take(do_ch.at[chunk], do_sem.at[chunk])

        def one(idx, carry_ch):
            da_ch[chunk, idx] = mm(do_ch[chunk, idx], b_ch[idx]).astype(BF16)
            return carry_ch
        lax.fori_loop(0, part, one, 0)
        exchange(lambda peer: da_ch.at[chunk, :, pl.ds(peer * CHUNK, CHUNK), :],
                 da_row.at[chunk, pl.ds(me * part, part)], 4, da_sem.at[chunk])
        return carry

    lax.fori_loop(0, n_chunk, da_chunk, 0)

    def db_one(idx, carry):
        total = mm_tn(do_ch[0, idx], a_ch[0, idx])
        for chunk in range(1, n_chunk):
            total += mm_tn(do_ch[chunk, idx], a_ch[chunk, idx])
        db_ch[idx] = total.astype(BF16)
        return carry

    lax.fori_loop(0, part, db_one, 0)

    def db_send(chunk, span, sem):
        exchange(lambda peer: db_ch.at[:, pl.ds(peer * rows + chunk * CHUNK, CHUNK), whole(span)],
                 db_row.at[chunk, pl.ds(me * part, part), :, whole(span)], 5, sem)

    last = n_chunk - 1
    for chunk in range(last):
        db_send(chunk, everything, db_sem.at[chunk])
    for tile in range(tiles):
        db_send(last, (tile, tile + 1), db_sem.at[last + tile])
    share_sum(0)

    def half_back(row, r_in, stage, blk, zn_t, span):
        grad = get_row(stage, r_in, span) * mask_of(row, span)
        proj = piece_of(blk, zn_t)
        sig = jax.nn.sigmoid(piece_of(blk + 2, zn_t))
        d_proj = grad * sig
        d_sig = d_proj * proj * (1.0 - sig)
        grow(2 + 2 * blk, mm_nt(zn_t, d_proj.astype(BF16)))
        grow(3 + 2 * blk, mm_nt(zn_t, d_sig.astype(BF16)))
        v_acc[4 + 2 * blk] += lane_fold(d_proj)
        v_acc[5 + 2 * blk] += lane_fold(d_sig)
        return (mm(w_in_ref[:, blk * chan:(blk + 1) * chan], d_proj.astype(BF16))
                + mm(w_in_ref[:, (blk + 2) * chan:(blk + 3) * chan], d_sig.astype(BF16)))

    def early_chunk(chunk, carry):
        take(da_row.at[chunk], da_sem.at[chunk])
        spread(stage_a, da_row.at[chunk], everything)

        def one_row(r_in, carry_row):
            row = chunk * CHUNK + r_in
            dzn_keep[row] = mm(w_gate_ref[...], gg_keep[row]) + half_back(row, r_in, stage_a, 0, zn_keep[row], everything)
            return carry_row
        lax.fori_loop(0, CHUNK, one_row, 0)
        return carry

    lax.fori_loop(0, n_chunk, early_chunk, 0)
    share_out(1, (0, 1, 2, 3, 4, 5))

    def late_piece(chunk, span):
        spread(stage_b, db_row.at[chunk], span)

        def one_row(r_in, carry_row):
            row = chunk * CHUNK + r_in
            zn_t = zn_keep[row, :, whole(span)]
            d_znorm = (dzn_keep[row, :, whole(span)] + half_back(row, r_in, stage_b, 1, zn_t, span)).astype(BF16).astype(F32)
            in_hat, in_inv = input_norm(row, span)
            v_acc[8] += lane_fold(d_znorm * in_hat)
            v_acc[9] += lane_fold(d_znorm)
            dz_t = mm_nt(eye[...], dy_ref[row, whole(span), :]) + norm_back(d_znorm * col(5), in_hat, in_inv)
            dz_ref[row, whole(span), :] = jnp.transpose(dz_t).astype(BF16)
            return carry_row
        lax.fori_loop(0, CHUNK, one_row, 0)

    def late_chunk(chunk, carry):
        take(db_row.at[chunk], db_sem.at[chunk])
        late_piece(chunk, everything)
        store_dz(chunk).start()
        return carry

    lax.fori_loop(0, last, late_chunk, 0)
    for tile in range(tiles):
        span = (tile, tile + 1)
        take(db_row.at[last, :, :, whole(span)], db_sem.at[last + tile])
        late_piece(last, span)
    share_out(2, (6, 7, 8, 9))
    store_dz(last).start()
    share_sum(1)
    share_sum(2)
    take(g_all, g_sem)
    for pos, blk in enumerate((4, 5, 0, 2, 1, 3)):
        gmat_ref[:, blk * chan:(blk + 1) * chan] = g_all[pos * chan:(pos + 1) * chan, :]

    others = (n_dev - 1) * part
    for sent, ref in ((0, b_send), (1, a_send), (3, do_send), (2, o_row), (4, da_row), (5, db_row)):
        take(ref.at[:, pl.ds(0, others)], send_sem.at[sent])
    take(m_recv.at[:, pl.ds(0, n_dev - 1)], send_sem.at[6])
    take(v_recv.at[:, pl.ds(0, n_dev - 1)], send_sem.at[7])
    take(g_all.at[pl.ds(0, 3 * (n_dev - 1) * shard)], send_sem.at[8])
    for chunk in range(n_chunk):
        store_dz(chunk).wait()


def finish(dz_in, gmat_ref, gvec_ref, dz_out, gw_in_ref, gw_gate_ref, gw_out_ref, b_in_ref, b_gate_ref, in_scale_ref, in_offset_ref,
           out_scale_ref, out_offset_ref, b_out_ref, hold, in_sem, out_sem):
    rows, _, chan = hold.shape
    n_chunk = rows // CHUNK

    def pull(chunk):
        span = pl.ds(chunk * CHUNK, CHUNK)
        return pltpu.make_async_copy(dz_in.at[span], hold.at[span], in_sem.at[chunk])

    def push(chunk):
        span = pl.ds(chunk * CHUNK, CHUNK)
        return pltpu.make_async_copy(hold.at[span], dz_out.at[span], out_sem.at[chunk])

    for chunk in range(n_chunk):
        pull(chunk).start()
    gw_in_ref[...] = gmat_ref[:, :4 * chan]
    gw_gate_ref[...] = gmat_ref[:, 4 * chan:5 * chan]
    gw_out_ref[...] = gmat_ref[:, 5 * chan:]
    b_gate_ref[...] = gvec_ref[0, 0:1, :]
    b_out_ref[...] = gvec_ref[0, 1:2, :]
    out_scale_ref[...] = gvec_ref[0, 2:3, :]
    out_offset_ref[...] = gvec_ref[0, 3:4, :]
    b_in_ref[0:1, :] = gvec_ref[0, 4:5, :]
    b_in_ref[2:3, :] = gvec_ref[0, 5:6, :]
    b_in_ref[1:2, :] = gvec_ref[1, 0:1, :]
    b_in_ref[3:4, :] = gvec_ref[1, 1:2, :]
    in_scale_ref[...] = gvec_ref[1, 2:3, :]
    in_offset_ref[...] = gvec_ref[1, 3:4, :]
    for chunk in range(n_chunk):
        pull(chunk).wait()
        push(chunk).start()
    for chunk in range(n_chunk):
        push(chunk).wait()


def local_grads(n_dev, z_loc, mask_loc, dy_loc, ln_in_scale, ln_in_offset, w_in, b_in, ln_out_scale, ln_out_offset, w_out, b_out, w_gate, b_gate):
    rows, num, chan = z_loc.shape
    n_chunk = rows // CHUNK
    part = chan // n_dev
    tiles = num // 128
    shard = 2 * chan // n_dev
    params = [vec.reshape(-1, chan) for vec in (b_in, b_gate, ln_in_scale, ln_in_offset, ln_out_scale, ln_out_offset, b_out)]
    vmem = pl.BlockSpec(memory_space=pltpu.VMEM)
    hbm = pl.BlockSpec(memory_space=pl.ANY)
    shapes = [jax.ShapeDtypeStruct((rows, num, chan), BF16), jax.ShapeDtypeStruct((chan, 6 * chan), BF16), jax.ShapeDtypeStruct((2, 8, chan), BF16)]
    pair = pltpu.VMEM((rows, num, chan), BF16)
    by_row = pltpu.VMEM((n_chunk, chan, CHUNK, num), BF16)
    by_chan = pltpu.VMEM((n_chunk, part, n_dev * CHUNK, num), BF16)
    by_chan_all = pltpu.VMEM((part, num, num), BF16)
    stage = pltpu.VMEM((tiles, chan * CHUNK, 128), F32)
    keep = pltpu.VMEM((rows, chan, num), BF16)
    square = pltpu.VMEM((chan, chan), BF16)
    dma = pltpu.SemaphoreType.DMA
    scratch = [
        pair, pair, pair, pltpu.VMEM((4 * chan, chan), BF16), square, square, square,
        pltpu.VMEM((chan, chan), F32), pltpu.VMEM((chan, chan), F32),
        by_row, by_row, by_chan, by_chan_all,
        pltpu.VMEM((n_chunk, part, n_dev * CHUNK, num), F32), pltpu.VMEM((n_chunk, chan, CHUNK, num), F32),
        by_row, by_chan, by_chan, by_row, by_chan_all, by_row,
        stage, stage, keep, keep, pltpu.VMEM((rows, chan, num), F32),
        pltpu.VMEM((6 * chan, chan), F32), pltpu.VMEM((10, chan, chan), F32), pltpu.VMEM((2, 8, chan), F32),
        pltpu.VMEM((3, n_dev, shard, chan), F32), pltpu.VMEM((2, n_dev, 8, chan), F32),
        pltpu.VMEM((3, shard, chan), BF16), pltpu.VMEM((6 * chan, chan), BF16),
        dma((n_chunk,)), dma, dma((n_chunk,)), dma((9,)),
        dma((n_chunk,)), dma, dma((n_chunk,)), dma((n_chunk,)), dma((n_chunk,)), dma((n_chunk - 1 + tiles,)),
        dma((3,)), dma((2,)), dma,
    ]
    d_z, gmat, gvec = pl.pallas_call(
        functools.partial(kernel, n_dev),
        out_shape=shapes,
        in_specs=[hbm, hbm] + [vmem] * 11,
        out_specs=[hbm, vmem, vmem],
        scratch_shapes=scratch,
        compiler_params=pltpu.CompilerParams(collective_id=0, has_side_effects=True, vmem_limit_bytes=67000000),
        name='triangle_backward',
    )(z_loc, dy_loc, mask_loc, w_in, w_gate, w_out, *params)
    row = jax.ShapeDtypeStruct((1, chan), BF16)
    square_out = jax.ShapeDtypeStruct((chan, chan), BF16)
    outs = pl.pallas_call(
        finish,
        out_shape=[shapes[0], jax.ShapeDtypeStruct((chan, 4 * chan), BF16), square_out, square_out, jax.ShapeDtypeStruct((4, chan), BF16)] + [row] * 6,
        in_specs=[hbm, vmem, vmem],
        out_specs=[hbm] + [vmem] * 10,
        scratch_shapes=[pair, dma((n_chunk,)), dma((n_chunk,))],
        name='write_outputs',
    )(d_z, gmat, gvec)
    d_z, gw_in, gw_gate, gw_out = outs[:4]
    d_b_in, d_b_gate, d_in_scale, d_in_offset, d_out_scale, d_out_offset, d_b_out = [vec.reshape(-1) for vec in outs[4:]]
    return (d_z, d_in_scale, d_in_offset, gw_in, d_b_in, d_out_scale, d_out_offset, gw_out, d_b_out, gw_gate, d_b_gate)


def solution(mesh):
    n_dev = mesh.shape['dap']
    pair_spec = P(('batch', 'dap'), None, None)
    mask_spec = P(('batch', 'dap'), None)
    vec_rep = P(None)
    mat_rep = P(None, None)
    vec_part = P('batch')
    mat_part = P('batch', None)
    in_specs = (pair_spec, mask_spec, pair_spec, vec_rep, vec_rep, mat_rep, vec_rep, vec_rep, vec_rep, mat_rep, vec_rep, mat_rep, vec_rep)
    out_specs = (pair_spec, vec_part, vec_part, mat_part, vec_part, vec_part, vec_part, mat_part, vec_part, mat_part, vec_part)
    return jax.shard_map(functools.partial(local_grads, n_dev), mesh=mesh, in_specs=in_specs, out_specs=out_specs, check_vma=False)
```
